256 devices in a mesh: gx: 8 (over z), gy: 4 (over x), gz: 8 (over y, core).
Axes of the slice: x: 4, y: 4, z: 8, core: 2. Of those that a mesh axis runs over, the one named last changes fastest.
Arguments:
- grads: float32 [256, 1, 1048576], P(('gx', 'gy', 'gz')), may hold values from -650 to 650
- loss_scale: float32 [], replicated, may hold values from 8 to 64
Outputs:
- clipped: float32 [1, 1048576], P(None, ('gx', 'gy', 'gz'))
- grad_norm: float32 [], replicated
The draws below stay inside these ranges and needn't reach their ends.
All inputs are finite; a program needn't handle non-finite values.
Results may differ from the reference program's by a relative error of at most 0.00002.
Values sent between devices are 32-bit elements; how exact they have to be, the bound alone decides.
A program may use at most 64 MiB of HBM per device.

```python
import math
import jax
import jax.numpy as jnp
from jax import lax

BUCKET = 1048576
BUCKETS = 1
REPLICAS = 256


def draw_grads(key, part):
    keys = jax.random.split(jax.random.fold_in(key, 17), 3)
    columns = jnp.arange(BUCKET, dtype=jnp.float32)
    rising = jnp.sqrt(1.0 + 2.0 * columns / BUCKET)
    colscale = jnp.exp(jax.random.uniform(keys[1], (BUCKETS, BUCKET), jnp.float32) * jnp.log(10.0))
    width = BUCKET // REPLICAS
    pairing = jax.random.permutation(keys[2], REPLICAS)
    block = jnp.arange(BUCKET, dtype=jnp.int32) // width
    spike = jnp.where(block[None, None, :] == pairing[:, None, None], 6.0, 1.0)
    values = jnp.clip(jax.random.normal(keys[0], (REPLICAS, BUCKETS, BUCKET), jnp.float32), -6.0, 6.0)
    return (values * (colscale * rising)[None] * spike).astype(jnp.float32)


def setup_inputs(seed: int = 0) -> dict:
    streams_of = jax.random.split(jax.random.key(seed), 3)
    return {
        "grads": draw_grads(jax.random.fold_in(streams_of[2], 71), 0),
        "loss_scale": jnp.clip(jnp.exp(jax.random.uniform(streams_of[1], (), jnp.float32, math.log(8.0), math.log(64.0))), 8.0, 64.0),
    }


def reference(grads, loss_scale):

    def accumulate(carry, item):
        return (carry + item, None)
    total, unused = lax.scan(accumulate, jnp.zeros((BUCKETS, BUCKET), jnp.float32), grads)
    unscaled = total / loss_scale
    grad_norm = jnp.sqrt(jnp.sum(unscaled * unscaled))
    factor = jnp.minimum(1.0, 0.5 * jnp.sqrt(jnp.float32(BUCKETS * BUCKET)) / (grad_norm + 1e-06))
    return (unscaled * factor, grad_norm)
```

```python
import jax
import jax.numpy as jnp
from jax import lax
from jax.experimental import pallas as pl
from jax.experimental.pallas import tpu as pltpu
from jax.sharding import Mesh
from jax.sharding import PartitionSpec as P

AXES = ("gx", "gy", "gz_0", "gz_1")
MESH = pl.DeviceIdType.MESH
TILE = 8
LANES = 128
SHARE = 32
RING = 24
PLANE = SHARE - RING

BLOCKS = (
    ("p", 2, 2), ("p", 2, 3), ("c", 4), ("p", 2, 1), ("p", 2, 0), ("c", 3), ("c", 5),
    ("p", 1, 3), ("p", 3, 2), ("p", 1, 0), ("p", 3, 1), ("c", 2), ("c", 6),
    ("p", 1, 2), ("p", 3, 3), ("p", 1, 1), ("p", 3, 0), ("c", 1), ("c", 7),
    ("p", 0, 2), ("p", 0, 3), ("p", 0, 1), ("p", 0, 0), ("c", 0),
)


class Names:
    def __init__(self):
        self.numbers = {}

    def __getitem__(self, name):
        return self.numbers.setdefault(name, len(self.numbers))


MESSAGES = 112


def kernel(
    g, scale, out, norm,
    pown, ppeer, cown, cpeer, prp, prm, pdp, pdm, p2rp, p2rm, p2dp, p2dm, pt, p3, crp, crm, cpl,
    nrow, nplane, zrow, nz, load_sem, send_sem, recv_sem, plane_send, plane_recv,
):
    z, x, y, c = (lax.axis_index(a) for a in AXES)
    names = Names()
    pending = []

    def ring_at(u, v, core):
        return u + core * (v - u), v + core * (u - v)

    p, q = ring_at(x, y, c)
    other = 1 - c

    def copy(name, src, dst, device):
        n = names[name]
        return pltpu.make_async_remote_copy(
            src_ref=src, dst_ref=dst, send_sem=send_sem.at[n], recv_sem=recv_sem.at[n],
            device_id=device, device_id_type=MESH,
        )

    def send(name, src, dst, device):
        message = copy(name, src, dst, device)
        message.start()
        pending.append(message)

    def wait(name, dst):
        copy(name, dst, dst, (z, x, y, other)).wait_recv()

    def along(u, v, zz):
        xx, yy = ring_at(lax.rem(p + u, 4), lax.rem(q + v, 4), c)
        return (lax.rem(z + zz, 8), xx, yy, c)

    u_next, u_back = along(1, 0, 0), along(3, 0, 0)
    v_next, v_back = along(0, 1, 0), along(0, 3, 0)
    z_next, z_back = along(0, 0, 1), along(0, 0, 7)
    partner = (z, x, y, other)

    def source(block, core):
        if block[0] == "p":
            pp, qq = ring_at(x, y, core)
            xx, yy = ring_at(lax.rem(pp + block[1], 4), lax.rem(qq + block[2], 4), core)
            return g.at[:, xx, yy, core, pl.ds(0, RING)]
        return g.at[lax.rem(z + block[1], 8), :, :, core, pl.ds(RING, PLANE)]

    def place(block, first, second):
        return first.at[block[1], block[2]] if block[0] == "p" else second.at[block[1]]

    loads = {}
    for n, block in enumerate(BLOCKS):
        loads[block] = pltpu.make_async_copy(source(block, c), place(block, pown, cown), load_sem.at[n])
        loads[block].start()

    barrier = pltpu.get_barrier_semaphore()
    greeted = (partner, u_next, u_back, v_next, v_back, z_next, z_back)
    for device in greeted:
        pl.semaphore_signal(barrier, inc=1, device_id=device, device_id_type=MESH)
    pl.semaphore_wait(barrier, len(greeted))

    for block in BLOCKS:
        send(("core", block), source(block, other), place(block, ppeer, cpeer), partner)

    def both(block):
        loads[block].wait()
        wait(("core", block), place(block, ppeer, cpeer))
        if block[0] == "p":
            _, k, j = block
            pown[k, j] = pown[k, j] + ppeer[k, j]
        else:
            k = block[1]
            cown[k] = cown[k] + cpeer[k]

    def half(h):
        return pl.ds(2 * h, 2)

    def c_up(m, h):
        send(("c+", m, h), cown.at[5 - m, half(h)], crp.at[m - 1, half(h)], z_next)

    def c_down(m, h):
        send(("c-", m, h), cown.at[3 + m, half(h)], crm.at[m - 1, half(h)], z_back)

    def c_up_arrived(m, h):
        wait(("c+", m, h), crp.at[m - 1, half(h)])
        k = 4 - m
        cown[k, half(h)] = cown[k, half(h)] + crp[m - 1, half(h)]

    def c_down_arrived(m, h):
        wait(("c-", m, h), crm.at[m - 1, half(h)])
        k = (4 + m) % 8
        cown[k, half(h)] = cown[k, half(h)] + crm[m - 1, half(h)]

    def d_up(j):
        send(("d+", j), pown.at[1, j], pdp.at[j], u_next)

    def d_down(j):
        send(("d-", j), pown.at[3, j], pdm.at[j], u_back)

    def r_up(i, j):
        send(("r+", i), pown.at[2, j], prp.at[i], u_next)

    def r_down(i, j):
        send(("r-", i), pown.at[2, j], prm.at[i], u_back)

    after = {
        ("p", 2, 2): lambda: r_up(0, 2),
        ("p", 2, 3): lambda: r_down(0, 3),
        ("p", 2, 1): lambda: r_up(1, 1),
        ("p", 2, 0): lambda: r_down(1, 0),
        ("c", 4): lambda: (c_up(1, 0), c_down(1, 1)),
        ("c", 3): lambda: c_up(2, 1),
        ("c", 5): lambda: c_down(2, 0),
        ("p", 1, 3): lambda: d_up(3),
        ("p", 3, 2): lambda: d_down(2),
        ("p", 1, 0): lambda: d_up(0),
        ("p", 3, 1): lambda: d_down(1),
    }
    for block in BLOCKS:
        both(block)
        if block in after:
            after[block]()

    def c_relay(m):
        for h in (1, 0) if m > 1 else (0,):
            c_up_arrived(m, h)
            if m < 4:
                c_up(m + 1, h)
        for h in (0, 1) if m > 1 else (1,):
            c_down_arrived(m, h)
            if m < 4:
                c_down(m + 1, h)

    def r_relay(i, up, down):
        wait(("r+", i), prp.at[i])
        pown[1, up] = pown[1, up] + prp[i]
        d_up(up)
        wait(("r-", i), prm.at[i])
        pown[3, down] = pown[3, down] + prm[i]
        d_down(down)

    def ring_sum(j):
        wait(("d+", j), pdp.at[j])
        wait(("d-", j), pdm.at[j])
        pown[0, j] = pown[0, j] + pdp[j] + pdm[j]

    c_relay(1)
    r_relay(0, 2, 3)
    r_relay(1, 1, 0)
    c_relay(2)

    low, high = pl.ds(0, 4), pl.ds(4, 4)
    ring_sum(2)
    send(("r2+",), pown.at[0, 2, low], p2rp, v_next)
    send(("r2-",), pown.at[0, 2, high], p2rm, v_back)
    ring_sum(3)
    send(("d2-", 0), pown.at[0, 3, low], p2dm.at[low], v_back)
    ring_sum(1)
    send(("d2+", 1), pown.at[0, 1, high], p2dp.at[high], v_next)
    c_relay(3)
    ring_sum(0)
    wait(("r2+",), p2rp)
    pown[0, 1, low] = pown[0, 1, low] + p2rp[...]
    send(("d2+", 0), pown.at[0, 1, low], p2dp.at[low], v_next)
    wait(("r2-",), p2rm)
    pown[0, 3, high] = pown[0, 3, high] + p2rm[...]
    send(("d2-", 1), pown.at[0, 3, high], p2dm.at[high], v_back)
    c_relay(4)
    for h in (0, 1):
        part = (low, high)[h]
        wait(("d2+", h), p2dp.at[part])
        wait(("d2-", h), p2dm.at[part])
    pt[...] = pown[0, 0] + p2dp[...] + p2dm[...]

    for d in (4, 3, 5, 2, 6, 1, 7):
        target = along(0, 0, d)
        send(("z", d), pt.at[target[0]], p3.at[d], target)
    for a in range(4):
        for b in range(4):
            if a or b:
                xx, yy = lax.rem(x + a, 4), lax.rem(y + b, 4)
                send(("xy", a, b), cown.at[0, xx, yy], cpl.at[4 * a + b], (z, xx, yy, c))

    mine = cown[0, x, y]
    for a in range(4):
        for b in range(4):
            if a or b:
                wait(("xy", a, b), cpl.at[4 * a + b])
                mine = mine + cpl[4 * a + b]
    ours = pt[z]
    for d in (1, 7, 2, 6, 3, 5, 4):
        wait(("z", d), p3.at[d])
        ours = ours + p3[d]
    divisor = scale[0, 0]
    ours = ours / divisor
    mine = mine / divisor

    squares = mine * mine
    for t in range(RING // TILE):
        piece = ours[TILE * t : TILE * (t + 1)]
        squares = squares + piece * piece
    row = jnp.sum(squares, axis=0, keepdims=True)
    nrow[...] = row
    slot = 8 * x + 2 * y + c
    nplane[slot] = row
    for a in range(4):
        for b in range(4):
            for e in range(2):
                if a or b or e:
                    device = (z, lax.rem(x + a, 4), lax.rem(y + b, 4), lax.rem(c + e, 2))
                    message = pltpu.make_async_remote_copy(
                        src_ref=nrow, dst_ref=nplane.at[slot], send_sem=plane_send, recv_sem=plane_recv,
                        device_id=device, device_id_type=MESH,
                    )
                    message.start()
    others = nplane.at[pl.ds(0, 31)]
    pltpu.make_async_copy(others, others, plane_recv).wait()
    row = jnp.sum(nplane[...], axis=0)
    zrow[...] = row
    nz[z] = row
    for d in (4, 3, 5, 2, 6, 1, 7):
        target = along(0, 0, d)
        send(("nz", d), zrow, nz.at[z], target)
    for d in (1, 7, 2, 6, 3, 5, 4):
        wait(("nz", d), nz.at[lax.rem(z + 8 - d, 8)])
    total = jnp.sum(jnp.sum(nz[...], axis=0), axis=1, keepdims=True)
    length = jnp.sqrt(total)
    factor = jnp.minimum(1.0, 512.0 / (length + 1e-06))
    norm[...] = length
    out[0:RING] = ours * factor
    out[RING:SHARE] = mine * factor

    for message in pending:
        message.wait_send()
    pltpu.make_async_copy(others, others, plane_send).wait()
    assert len(names.numbers) <= MESSAGES, len(names.numbers)


def per_device(grads, loss_scale):
    blocks = grads.reshape(8, 4, 4, 2, SHARE, LANES)
    f32 = jnp.float32

    def vmem(*shape):
        return pltpu.VMEM((*shape, LANES), f32)

    clipped, norm = pl.pallas_call(
        kernel,
        name="reduce_clip",
        out_shape=(
            jax.ShapeDtypeStruct((SHARE, LANES), f32),
            jax.ShapeDtypeStruct((1, 1), f32),
        ),
        in_specs=[
            pl.BlockSpec(memory_space=pltpu.HBM),
            pl.BlockSpec(memory_space=pltpu.SMEM),
        ],
        out_specs=(
            pl.BlockSpec(memory_space=pltpu.VMEM),
            pl.BlockSpec(memory_space=pltpu.VMEM),
        ),
        scratch_shapes=[
            vmem(4, 4, 8, RING), vmem(4, 4, 8, RING),
            vmem(8, 4, 4, PLANE), vmem(8, 4, 4, PLANE),
            vmem(2, 8, RING), vmem(2, 8, RING),
            vmem(4, 8, RING), vmem(4, 8, RING),
            vmem(4, RING), vmem(4, RING),
            vmem(8, RING), vmem(8, RING),
            vmem(8, RING), vmem(8, RING),
            vmem(4, 4, 4, PLANE), vmem(4, 4, 4, PLANE),
            vmem(16, PLANE),
            vmem(1), vmem(32, 1), vmem(1), vmem(8, 1),
            pltpu.SemaphoreType.DMA((len(BLOCKS),)),
            pltpu.SemaphoreType.DMA((MESSAGES,)),
            pltpu.SemaphoreType.DMA((MESSAGES,)),
            pltpu.SemaphoreType.DMA,
            pltpu.SemaphoreType.DMA,
        ],
        compiler_params=pltpu.CompilerParams(collective_id=0, has_side_effects=True),
    )(blocks, loss_scale.reshape(1, 1))
    return clipped.reshape(1, SHARE * LANES), norm.reshape(())


def solution(mesh):
    torus = Mesh(mesh.devices.reshape(mesh.shape["gx"], mesh.shape["gy"], 4, 2), AXES)
    return jax.shard_map(
        per_device,
        mesh=torus,
        in_specs=(P(AXES, None, None), P()),
        out_specs=(P(None, AXES), P()),
        check_vma=False,
    )
```

```python
import jax
import jax.numpy as jnp
from jax import lax
from jax.experimental import pallas as pl
from jax.experimental.pallas import tpu as pltpu
from jax.sharding import Mesh
from jax.sharding import PartitionSpec as P

AXES = ("gx", "gy", "gz_0", "gz_1")
MESH = pl.DeviceIdType.MESH
TILE = 8
LANES = 128
SHARE = 32
RING = 24
PLANE = SHARE - RING

BLOCKS = (
    ("p", 2, 2), ("p", 2, 3), ("c", 4), ("p", 2, 1), ("p", 2, 0), ("c", 3), ("c", 5),
    ("p", 1, 3), ("p", 3, 2), ("p", 1, 0), ("p", 3, 1), ("c", 2), ("c", 6),
    ("p", 1, 2), ("p", 3, 3), ("p", 1, 1), ("p", 3, 0), ("c", 1), ("c", 7),
    ("p", 0, 2), ("p", 0, 3), ("p", 0, 1), ("p", 0, 0), ("c", 0),
)


class Names:
    def __init__(self):
        self.numbers = {}

    def __getitem__(self, name):
        return self.numbers.setdefault(name, len(self.numbers))


MESSAGES = 64
EACH = ("core", "r+", "r-", "d+", "d-", "c+", "c-", "r2+", "r2-", "d2+", "d2-")
SENT = (
    ("corep",), ("corec",), ("r+", "r-", "d+", "d-"), ("c+", "c-"), ("r2+", "r2-", "d2+", "d2-"), ("z",), ("xy",), ("nz",), ("plane",),
)


def kernel(
    g, scale, out, norm, scaled,
    pown, ppeer, cown, cpeer, prp, prm, pdp, pdm, p2rp, p2rm, p2dp, p2dm, pt, p3, crp, crm, cpl,
    nrow, nplane, zrow, nz, load_sem, send_sem, recv_sem,
):
    z, x, y, c = (lax.axis_index(a) for a in AXES)
    names = Names()
    kinds = {kind: n for n, group in enumerate(SENT) for kind in group}

    def ring_at(u, v, core):
        return u + core * (v - u), v + core * (u - v)

    p, q = ring_at(x, y, c)
    other = 1 - c

    def copy(name, src, dst, device):
        n = names[name if name[0] in EACH else name[:1]]
        kind = kinds[name[0] + name[1][0] if name[0] == "core" else name[0]]
        return pltpu.make_async_remote_copy(
            src_ref=src, dst_ref=dst, send_sem=send_sem.at[kind], recv_sem=recv_sem.at[n],
            device_id=device, device_id_type=MESH,
        )

    def send(name, src, dst, device):
        copy(name, src, dst, device).start()

    def arrived(name, whole):
        pltpu.make_async_copy(whole, whole, recv_sem.at[names[name]]).wait()

    def sent(kind, whole):
        pltpu.make_async_copy(whole, whole, send_sem.at[kinds[kind]]).wait()

    def wait(name, dst):
        copy(name, dst, dst, (z, x, y, other)).wait_recv()

    def along(u, v, zz):
        xx, yy = ring_at(lax.rem(p + u, 4), lax.rem(q + v, 4), c)
        return (lax.rem(z + zz, 8), xx, yy, c)

    u_next, u_back = along(1, 0, 0), along(3, 0, 0)
    v_next, v_back = along(0, 1, 0), along(0, 3, 0)
    z_next, z_back = along(0, 0, 1), along(0, 0, 7)
    partner = (z, x, y, other)

    def source(block, core):
        if block[0] == "p":
            pp, qq = ring_at(x, y, core)
            xx, yy = ring_at(lax.rem(pp + block[1], 4), lax.rem(qq + block[2], 4), core)
            return g.at[:, xx, yy, core, pl.ds(0, RING)]
        return g.at[lax.rem(z + block[1], 8), :, :, core, pl.ds(RING, PLANE)]

    def place(block, first, second):
        return first.at[block[1], block[2]] if block[0] == "p" else second.at[block[1]]

    for block in BLOCKS:
        pltpu.make_async_copy(source(block, c), place(block, pown, cown), load_sem.at[int(block[0] == "c")]).start()

    barrier = pltpu.get_barrier_semaphore()
    greeted = (partner, u_next, u_back, v_next, v_back, z_next, z_back)
    for device in greeted:
        pl.semaphore_signal(barrier, inc=1, device_id=device, device_id_type=MESH)
    pl.semaphore_wait(barrier, len(greeted))

    for block in BLOCKS:
        send(("core", block), source(block, other), place(block, ppeer, cpeer), partner)

    def both(block):
        wait(("core", block), place(block, ppeer, cpeer))
        if block[0] == "p":
            _, k, j = block
            pown[k, j] = pown[k, j] + ppeer[k, j]
        else:
            k = block[1]
            cown[k] = cown[k] + cpeer[k]

    def half(h):
        return pl.ds(2 * h, 2)

    def c_up(m, h):
        send(("c+", m, h), cown.at[5 - m, half(h)], crp.at[m - 1, half(h)], z_next)

    def c_down(m, h):
        send(("c-", m, h), cown.at[3 + m, half(h)], crm.at[m - 1, half(h)], z_back)

    def c_up_arrived(m, h):
        wait(("c+", m, h), crp.at[m - 1, half(h)])
        k = 4 - m
        cown[k, half(h)] = cown[k, half(h)] + crp[m - 1, half(h)]

    def c_down_arrived(m, h):
        wait(("c-", m, h), crm.at[m - 1, half(h)])
        k = (4 + m) % 8
        cown[k, half(h)] = cown[k, half(h)] + crm[m - 1, half(h)]

    def d_up(j):
        send(("d+", j), pown.at[1, j], pdp.at[j], u_next)

    def d_down(j):
        send(("d-", j), pown.at[3, j], pdm.at[j], u_back)

    def r_up(i, j):
        send(("r+", i), pown.at[2, j], prp.at[i], u_next)

    def r_down(i, j):
        send(("r-", i), pown.at[2, j], prm.at[i], u_back)

    after = {
        ("p", 2, 2): lambda: r_up(0, 2),
        ("p", 2, 3): lambda: r_down(0, 3),
        ("p", 2, 1): lambda: r_up(1, 1),
        ("p", 2, 0): lambda: r_down(1, 0),
        ("c", 4): lambda: (c_up(1, 0), c_down(1, 1)),
        ("c", 3): lambda: c_up(2, 1),
        ("c", 5): lambda: c_down(2, 0),
        ("p", 1, 3): lambda: d_up(3),
        ("p", 3, 2): lambda: d_down(2),
        ("p", 1, 0): lambda: d_up(0),
        ("p", 3, 1): lambda: d_down(1),
    }
    pltpu.make_async_copy(pown, pown, load_sem.at[0]).wait()
    pltpu.make_async_copy(cown, cown, load_sem.at[1]).wait()
    for block in BLOCKS:
        both(block)
        if block in after:
            after[block]()

    def c_relay(m):
        for h in (1, 0) if m > 1 else (0,):
            c_up_arrived(m, h)
            if m < 4:
                c_up(m + 1, h)
        for h in (0, 1) if m > 1 else (1,):
            c_down_arrived(m, h)
            if m < 4:
                c_down(m + 1, h)

    def r_relay(i, up, down):
        wait(("r+", i), prp.at[i])
        pown[1, up] = pown[1, up] + prp[i]
        d_up(up)
        wait(("r-", i), prm.at[i])
        pown[3, down] = pown[3, down] + prm[i]
        d_down(down)

    def ring_sum(j):
        wait(("d+", j), pdp.at[j])
        wait(("d-", j), pdm.at[j])
        pown[0, j] = pown[0, j] + pdp[j] + pdm[j]

    c_relay(1)
    r_relay(0, 2, 3)
    r_relay(1, 1, 0)
    c_relay(2)

    low, high = pl.ds(0, 4), pl.ds(4, 4)
    ring_sum(2)
    send(("r2+",), pown.at[0, 2, low], p2rp, v_next)
    send(("r2-",), pown.at[0, 2, high], p2rm, v_back)
    ring_sum(3)
    send(("d2-", 0), pown.at[0, 3, low], p2dm.at[low], v_back)
    ring_sum(1)
    send(("d2+", 1), pown.at[0, 1, high], p2dp.at[high], v_next)
    c_relay(3)
    ring_sum(0)
    wait(("r2+",), p2rp)
    pown[0, 1, low] = pown[0, 1, low] + p2rp[...]
    send(("d2+", 0), pown.at[0, 1, low], p2dp.at[low], v_next)
    wait(("r2-",), p2rm)
    pown[0, 3, high] = pown[0, 3, high] + p2rm[...]
    send(("d2-", 1), pown.at[0, 3, high], p2dm.at[high], v_back)
    c_relay(4)
    for h in (0, 1):
        part = (low, high)[h]
        wait(("d2+", h), p2dp.at[part])
        wait(("d2-", h), p2dm.at[part])
    pt[...] = pown[0, 0] + p2dp[...] + p2dm[...]

    for d in (4, 3, 5, 2, 6, 1, 7):
        target = along(0, 0, d)
        send(("z", d), pt.at[target[0]], p3.at[d], target)
    for a in range(4):
        for b in range(4):
            if a or b:
                xx, yy = lax.rem(x + a, 4), lax.rem(y + b, 4)
                send(("xy", a, b), cown.at[0, xx, yy], cpl.at[4 * a + b], (z, xx, yy, c))

    arrived(("xy",), cpl.at[pl.ds(1, 15)])
    mine = cown[0, x, y]
    for a in range(4):
        for b in range(4):
            if a or b:
                mine = mine + cpl[4 * a + b]
    arrived(("z",), p3.at[pl.ds(1, 7)])
    ours = pt[z]
    for d in (1, 7, 2, 6, 3, 5, 4):
        ours = ours + p3[d]
    divisor = scale[0, 0]
    ours = ours / divisor
    mine = mine / divisor
    out[0:RING] = ours
    out[RING:SHARE] = mine

    squares = mine * mine
    for t in range(RING // TILE):
        piece = ours[TILE * t : TILE * (t + 1)]
        squares = squares + piece * piece
    row = jnp.sum(squares, axis=0, keepdims=True)
    nrow[...] = row
    slot = 8 * x + 2 * y + c
    nplane[slot] = row
    for a in range(4):
        for b in range(4):
            for e in range(2):
                if a or b or e:
                    device = (z, lax.rem(x + a, 4), lax.rem(y + b, 4), lax.rem(c + e, 2))
                    send(("plane",), nrow, nplane.at[slot], device)
    others = nplane.at[pl.ds(0, 31)]
    arrived(("plane",), others)
    row = jnp.sum(nplane[...], axis=0)
    zrow[...] = row
    nz[z] = row
    for d in (4, 3, 5, 2, 6, 1, 7):
        target = along(0, 0, d)
        send(("nz", d), zrow, nz.at[z], target)
    arrived(("nz",), nz.at[pl.ds(0, 7)])
    total = jnp.sum(jnp.sum(nz[...], axis=0), axis=1, keepdims=True)
    length = jnp.sqrt(total)
    factor = jnp.minimum(1.0, 512.0 / (length + 1e-06))
    norm[...] = length
    scaled[...] = jnp.broadcast_to(factor, (1, LANES))

    sent("corep", ppeer)
    sent("corec", cpeer)
    sent("r+", pown.at[pl.ds(0, 3)])
    sent("c+", cown.at[pl.ds(0, 7)])
    sent("r2+", pown.at[0, pl.ds(0, 3)])
    sent("z", p3.at[pl.ds(1, 7)])
    sent("xy", cpl.at[pl.ds(1, 15)])
    sent("plane", others)
    sent("nz", nz.at[pl.ds(0, 7)])
    assert len(names.numbers) <= MESSAGES, len(names.numbers)


def per_device(grads, loss_scale):
    blocks = grads.reshape(8, 4, 4, 2, SHARE, LANES)
    f32 = jnp.float32

    def vmem(*shape):
        return pltpu.VMEM((*shape, LANES), f32)

    unscaled, norm, factor = pl.pallas_call(
        kernel,
        name="reduce_clip",
        out_shape=(vmem(SHARE), pltpu.VMEM((1, 1), f32), vmem(1)),
        in_specs=[
            pl.BlockSpec(memory_space=pltpu.HBM),
            pl.BlockSpec(memory_space=pltpu.SMEM),
        ],
        out_specs=(pl.BlockSpec(memory_space=pltpu.VMEM),) * 3,
        scratch_shapes=[
            vmem(4, 4, 8, RING), vmem(4, 4, 8, RING),
            vmem(8, 4, 4, PLANE), vmem(8, 4, 4, PLANE),
            vmem(2, 8, RING), vmem(2, 8, RING),
            vmem(4, 8, RING), vmem(4, 8, RING),
            vmem(4, RING), vmem(4, RING),
            vmem(8, RING), vmem(8, RING),
            vmem(8, RING), vmem(8, RING),
            vmem(4, 4, 4, PLANE), vmem(4, 4, 4, PLANE),
            vmem(16, PLANE),
            vmem(1), vmem(32, 1), vmem(1), vmem(8, 1),
            pltpu.SemaphoreType.DMA((2,)),
            pltpu.SemaphoreType.DMA((len(SENT),)),
            pltpu.SemaphoreType.DMA((MESSAGES,)),
        ],
        compiler_params=pltpu.CompilerParams(collective_id=0, has_side_effects=True),
    )(blocks, loss_scale.reshape(1, 1))
    return (unscaled * factor).reshape(1, SHARE * LANES), norm.reshape(())


def solution(mesh):
    torus = Mesh(mesh.devices.reshape(mesh.shape["gx"], mesh.shape["gy"], 4, 2), AXES)
    return jax.shard_map(
        per_device,
        mesh=torus,
        in_specs=(P(AXES, None, None), P()),
        out_specs=(P(None, AXES), P()),
        check_vma=False,
    )
```
